32 devices in a mesh: dp: 4 (over z), rows: 8 (over y, x, core).
Axes of the slice: x: 2, y: 2, z: 4, core: 2. Of those that a mesh axis runs over, the one named last changes fastest.
Arguments:
- owners: int32 [32768, 1], P(('dp', 'rows')), may hold values from 0 to 31; in each aligned block of 1024 rows (0 to 1023, 1024 to 2047, ...) at most 128 rows name the same one
- offsets: int32 [32768], P(('dp', 'rows')), may hold values from 0 to 8191
- gradients: bfloat16 [32768, 128], P(('dp', 'rows')), may hold values from -6 to 6
- embedding: float32 [262144, 128], P(('dp', 'rows')), may hold values from -6 to 6
- adagrad_state: float32 [262144], P(('dp', 'rows')), may hold values from 0.05 to 2
- next_owners: int32 [32768, 1], P(('dp', 'rows')), may hold values from 0 to 31; in each aligned block of 1024 rows (0 to 1023, 1024 to 2047, ...) at most 128 rows name the same one
- next_offsets: int32 [32768], P(('dp', 'rows')), may hold values from 0 to 8191
Outputs:
- new_embedding: float32 [262144, 128], P(('dp', 'rows'))
- new_state: float32 [262144], P(('dp', 'rows'))
- next_rows: bfloat16 [32768, 128], P(('dp', 'rows'))
The draws below stay inside these ranges and needn't reach their ends.
Inputs may be any that keep to these rules, and one draw needn't show every extreme that they name: `owners`: within the 1024 rows of one device, at most 128 rows name the same block. `next_owners`: within the 1024 rows of one device, at most 128 rows name the same block.
All inputs are finite; a program needn't handle non-finite values.
Results may differ from the reference program's by a relative error of at most 0.0013.
Values may be sent and summed in bfloat16 or wider, within the bound.
A program may use at most 64 MiB of HBM per device.

```python
import math
import jax
import jax.numpy as jnp
import numpy as np
from jax import lax

W = 128
R_DEV = 8192
L_DEV = 1024
V = 262144
LOOKUPS = 32768
CAP = 128
N_DP = 4
N_ROWS = 8


def plant(result, own_key, low, top_value):
    longest = result.shape.index(max(result.shape))
    spots = []
    for shift in (0, 1):
        where = [jax.random.randint(jax.random.fold_in(own_key, axis), (), 0, length) for axis, length in enumerate(result.shape)]
        where[longest] = (where[longest] + shift) % result.shape[longest]
        spots.append(tuple(where))
    return result.at[spots[0]].set(low).at[spots[1]].set(top_value)


def levels(own_key, extent, cuts, least, top_value):
    gain, own = 1.0, jax.random.fold_in(own_key, 6)
    for position, parts in cuts:
        steps = jnp.exp(jax.random.uniform(jax.random.fold_in(own, position), (parts,), jnp.float32, least / len(cuts), top_value / len(cuts)))
        gain = gain * jnp.repeat(steps, extent[position] // parts).reshape([-1 if axis == position else 1 for axis in range(len(extent))])
    return gain


def cumulative_ranks(count, lean):
    loads = [(1 << 20) // math.isqrt(rank ** lean) + 1 for rank in range(1, count + 1)]
    deviation = 1 + sum(loads) // (1 << 30)
    return np.cumsum(np.array([max(1, weight // deviation) for weight in loads]))


def ranked_ids(rng, dims, count, slope):
    listing = cumulative_ranks(count, slope)
    ticket = jax.random.randint(jax.random.fold_in(rng, 1), dims, 0, int(listing[count - 1]))
    rank = jnp.searchsorted(jnp.asarray(listing, jnp.int32), ticket, side="right")
    return jax.random.permutation(jax.random.fold_in(rng, 2), count)[rank].astype(jnp.int32)


def deal_out(stream_key, own, number, rows, count, top, bound, skew):
    sequence = jax.random.permutation(stream_key, count)
    packed, common = portions_of(count, rows * top, bound, skew, True), portions_of(count, rows * top, bound, skew, False)
    places = jnp.arange(count)

    def named(lengths, rotation):
        used = int((lengths > 0).sum())
        fixed = max(1, used // 4)
        shifted = fixed + (places - fixed + rotation * (used - fixed)) % max(1, count - fixed)
        return jnp.zeros((count,), jnp.int32).at[sequence[jnp.where(places < fixed, places, shifted)]].set(jnp.asarray(lengths, jnp.int32))

    lengths = jnp.where(number % 4 == 0, named(packed, number // 4), named(common, number - number // 4 - 1))
    mixed = jax.random.permutation(jax.random.fold_in(own, 3), count)
    giver, receiver = mixed[0:count // 2 * 2:2], mixed[1:count // 2 * 2:2]
    room = jnp.minimum(lengths[giver] - 1, bound - lengths[receiver]) // 2
    room = jnp.where((giver == sequence[0]) | (receiver == sequence[0]) | (lengths[receiver] == 0), 0, jnp.maximum(room, 0))
    shifted = jax.random.randint(jax.random.fold_in(own, 4), (count // 2,), 0, 1 << 20) % (room + 1)
    lengths = lengths.at[giver].add(-shifted).at[receiver].add(shifted)
    items = jnp.searchsorted(jnp.cumsum(lengths), jnp.arange(rows * top), side="right").astype(jnp.int32)
    grid = items.reshape(top, rows).T
    grid = grid[jax.random.permutation(jax.random.fold_in(own, 1), rows)]
    rotation = jax.random.randint(jax.random.fold_in(own, 2), (rows, 1), 0, top)
    return jnp.take_along_axis(grid, (jnp.arange(top)[None, :] + rotation) % top, axis=1)


def portions_of(count, total, bound, lean, full):
    portions = [(1 << 20) // math.isqrt(standing ** lean) + 1 for standing in range(1, count + 1)]
    largest = bound if full else min(bound, max(-(-total // count), total * portions[0] // sum(portions)))
    least = 1 if total - largest >= count - 1 else 0
    counts, spare = [largest] + [least] * (count - 1), total - largest - least * (count - 1)
    while spare > 0:
        movable = [i for i in range(1, count) if counts[i] < largest] or [i for i in range(1, count) if counts[i] < bound]
        pool, budget = sum([portions[i] for i in movable]), spare
        for i in movable:
            extra = min(bound - counts[i], max(1, budget * portions[i] // pool), spare)
            counts[i] = counts[i] + extra
            spare = spare - extra
    return np.array(counts)


def centred(rng, dims, spread, most, cuts=(), dtype=jnp.bfloat16):
    values = jax.random.normal(rng, dims, jnp.float32) * spread
    if len(cuts) > 0:
        values = levels(rng, dims, cuts, -0.22, 0.18) * values
    return jnp.clip(values, min=-most, max=most).astype(dtype)


def setup_inputs(seed: int = 0) -> dict:
    key_list = jax.random.split(jax.random.key(seed), 8)
    owners_keys = jax.random.split(jax.random.fold_in(key_list[0], 1), LOOKUPS // L_DEV)
    owners_turns = jax.random.permutation(jax.random.fold_in(key_list[0], 3), LOOKUPS // L_DEV)
    owners = jax.vmap(lambda own, number: deal_out(jax.random.fold_in(key_list[0], 2), own, number, L_DEV, N_DP * N_ROWS, 1, CAP, 2))(owners_keys, owners_turns).reshape((LOOKUPS, 1))
    offsets = plant(ranked_ids(key_list[1], (LOOKUPS,), R_DEV, 2), jax.random.fold_in(key_list[1], 3), 0, R_DEV - 1).astype(jnp.int32)
    gradients = centred(key_list[2], (LOOKUPS, W), 1.0, 6.0, ((0, 32),))
    embedding = centred(key_list[3], (V, W), 1.0, 6.0, ((0, 32),), jnp.float32)
    adagrad_state = jnp.clip(jnp.exp(math.log(2.0) - 3.6888794 * jax.random.uniform(key_list[4], (V,), jnp.float32) ** levels(key_list[4], (V,), ((0, 32),), -0.2, 0.2)), 0.05, 2.0)
    next_owners_keys = jax.random.split(jax.random.fold_in(key_list[5], 1), LOOKUPS // L_DEV)
    next_owners_turns = jax.random.permutation(jax.random.fold_in(key_list[5], 3), LOOKUPS // L_DEV)
    next_owners = jax.vmap(lambda own, number: deal_out(jax.random.fold_in(key_list[5], 2), own, number, L_DEV, N_DP * N_ROWS, 1, CAP, 2))(next_owners_keys, next_owners_turns).reshape((LOOKUPS, 1))
    next_offsets = plant(ranked_ids(key_list[6], (LOOKUPS,), R_DEV, 2), jax.random.fold_in(key_list[6], 3), 0, R_DEV - 1).astype(jnp.int32)
    return {"owners": owners, "offsets": offsets, "gradients": gradients, "embedding": embedding, "adagrad_state": adagrad_state, "next_owners": next_owners, "next_offsets": next_offsets}


def reference(owners, offsets, gradients, embedding, adagrad_state, next_owners, next_offsets):
    row_ids = (owners[:, 0] * R_DEV + offsets).astype(jnp.int32)
    grad_sum = jnp.zeros((V, W), jnp.float32).at[row_ids].add(gradients.astype(jnp.float32))
    new_state = adagrad_state + lax.optimization_barrier(jnp.mean(grad_sum * grad_sum, axis=1))
    new_embedding = embedding - 0.5 * grad_sum / jnp.sqrt(new_state)[:, None]
    next_ids = (next_owners[:, 0] * R_DEV + next_offsets).astype(jnp.int32)
    next_rows = new_embedding[next_ids].astype(jnp.bfloat16)
    return (new_embedding, new_state, next_rows)
```

```python
import jax
import jax.numpy as jnp
from jax import lax
from jax.experimental import pallas as pl
from jax.experimental.pallas import tpu as pltpu
from jax.sharding import PartitionSpec as P

BANKS = 4
LANES = 128
BASE = 256


def place(owner_ids, offsets, devices, capacity):
    lookups = owner_ids.shape[0]
    one_hot = (owner_ids[:, None] == jnp.arange(devices, dtype=jnp.int32)[None, :]).astype(
        jnp.bfloat16
    )
    positions = jnp.arange(lookups, dtype=jnp.int32)
    earlier = (positions[:, None] > positions[None, :]).astype(jnp.bfloat16)
    ahead = jnp.dot(earlier, one_hot, preferred_element_type=jnp.float32)
    slot_ids = jnp.sum(ahead * one_hot.astype(jnp.float32), axis=1).astype(jnp.int32)
    in_slot = slot_ids[:, None] == jnp.arange(capacity, dtype=jnp.int32)[None, :]
    high = (offsets // BASE).astype(jnp.float32)[:, None]
    low = (offsets % BASE).astype(jnp.float32)[:, None]
    columns = jnp.concatenate(
        [jnp.where(in_slot, high, 0.0), jnp.where(in_slot, low, 0.0), jnp.where(in_slot, 1.0, 0.0)],
        axis=1,
    ).astype(jnp.bfloat16)
    table = lax.dot_general(
        one_hot, columns, (((0,), (0,)), ((), ())), preferred_element_type=jnp.float32
    ).astype(jnp.int32)
    high, low, used = jnp.split(table, 3, axis=1)
    return owner_ids * capacity + slot_ids, high * BASE + low, used


def update_kernel(
    rows_ref, wanted_ref, incoming_ref, embedding_ref, state_ref,
    new_embedding_ref, new_state_ref, fetched_ref,
    *scratch,
):
    banks = scratch[:BANKS]
    table, picked, in_sem, out_sems = scratch[BANKS:]
    owned = table.shape[0]
    slots = incoming_ref.shape[0]
    chunks = out_sems.shape[0]
    chunk = owned // chunks

    load = pltpu.make_async_copy(embedding_ref, table, in_sem)
    load.start()

    zero_rows = 64

    @pl.loop(0, owned // zero_rows)
    def _(step):
        for bank in banks:
            bank[pl.ds(pl.multiple_of(step * zero_rows, zero_rows), zero_rows), :] = jnp.zeros(
                (zero_rows, LANES), jnp.float32
            )

    group = 32

    @pl.loop(0, slots // group)
    def _(step):
        start = pl.multiple_of(step * group, group)
        block = incoming_ref[pl.ds(start, group), :].astype(jnp.float32)
        for first in range(0, group, BANKS):
            where = [rows_ref[start + first + k] for k in range(BANKS)]
            sums = [
                banks[k][pl.ds(where[k], 1), :] + block[first + k : first + k + 1, :]
                for k in range(BANKS)
            ]
            for k in range(BANKS):
                banks[k][pl.ds(where[k], 1), :] = sums[k]

    load.wait()
    for piece in range(chunks):

        @pl.loop(0, chunk // LANES)
        def _(step):
            tile = piece * (chunk // LANES) + step
            span = pl.ds(pl.multiple_of(tile * LANES, LANES), LANES)
            grad_sum = banks[0][span, :]
            for bank in banks[1:]:
                grad_sum = grad_sum + bank[span, :]
            mean = jnp.sum(grad_sum * grad_sum, axis=1, keepdims=True) * (1.0 / LANES)
            old = jnp.broadcast_to(state_ref[pl.ds(tile, 1), :], (LANES, LANES)).T
            state = old + mean
            new_state_ref[pl.ds(tile, 1), :] = state.T[0:1, :]
            table[span, :] = table[span, :] - 0.5 * grad_sum / jnp.sqrt(state)

        span = pl.ds(piece * chunk, chunk)
        pltpu.make_async_copy(
            table.at[span, :], new_embedding_ref.at[span, :], out_sems.at[piece]
        ).start()

    @pl.loop(0, slots // group)
    def _(step):
        start = pl.multiple_of(step * group, group)
        for k in range(group):
            picked[pl.ds(start + k, 1), :] = table[pl.ds(wanted_ref[start + k], 1), :]

    @pl.loop(0, slots // LANES)
    def _(step):
        span = pl.ds(pl.multiple_of(step * LANES, LANES), LANES)
        fetched_ref[span, :] = picked[span, :].astype(jnp.bfloat16)

    for piece in range(chunks):
        span = pl.ds(piece * chunk, chunk)
        pltpu.make_async_copy(
            table.at[span, :], new_embedding_ref.at[span, :], out_sems.at[piece]
        ).wait()


def update(rows, wanted, incoming, embedding, state):
    owned, columns = embedding.shape
    slots = incoming.shape[0]
    chunks = 8
    smem = pl.BlockSpec(memory_space=pltpu.SMEM)
    vmem = pl.BlockSpec(memory_space=pltpu.VMEM)
    hbm = pl.BlockSpec(memory_space=pl.ANY)
    new_embedding, new_state, fetched = pl.pallas_call(
        update_kernel,
        name="update",
        out_shape=(
            jax.ShapeDtypeStruct((owned, columns), jnp.float32),
            jax.ShapeDtypeStruct((owned // LANES, LANES), jnp.float32),
            jax.ShapeDtypeStruct((slots, columns), jnp.bfloat16),
        ),
        in_specs=[smem, smem, vmem, hbm, vmem],
        out_specs=(hbm, vmem, vmem),
        scratch_shapes=[pltpu.VMEM((owned + 8, columns), jnp.float32)] * BANKS
        + [
            pltpu.VMEM((owned, columns), jnp.float32),
            pltpu.VMEM((slots, columns), jnp.float32),
            pltpu.SemaphoreType.DMA,
            pltpu.SemaphoreType.DMA((chunks,)),
        ],
        compiler_params=pltpu.CompilerParams(vmem_limit_bytes=40 * 1024 * 1024),
    )(rows, wanted, incoming, embedding, state.reshape(owned // LANES, LANES))
    return new_embedding, new_state.reshape(owned), fetched


def on_device(owners, offsets, gradients, embedding, adagrad_state, next_owners, next_offsets):
    axes = ("dp", "rows")
    devices = lax.axis_size(axes)
    lookups, columns = gradients.shape
    owned_rows = embedding.shape[0]
    capacity = max(2, 4 * lookups // devices)
    slots = devices * capacity
    places, slot_rows, used = place(owners[:, 0], offsets, devices, capacity)
    next_places, requests, _ = place(next_owners[:, 0], next_offsets, devices, capacity)
    slot_rows = jnp.where(used > 0, slot_rows, owned_rows)
    ids = jnp.stack([slot_rows, requests], axis=1)
    ids = lax.all_to_all(ids, axes, split_axis=0, concat_axis=0, tiled=True)
    slot_index = jnp.arange(slots, dtype=jnp.int32)
    outgoing = jnp.dot(
        (slot_index[:, None] == places[None, :]).astype(jnp.bfloat16),
        gradients,
        preferred_element_type=jnp.float32,
    ).astype(jnp.bfloat16)
    incoming = lax.all_to_all(
        outgoing.reshape(devices, capacity, columns), axes, split_axis=0, concat_axis=0, tiled=True
    )
    new_embedding, new_state, fetched = update(
        ids[:, 0].reshape(-1), ids[:, 1].reshape(-1),
        incoming.reshape(slots, columns), embedding, adagrad_state,
    )
    returned = lax.all_to_all(
        fetched.reshape(devices, capacity, columns), axes, split_axis=0, concat_axis=0, tiled=True
    )
    next_rows = jnp.dot(
        (next_places[:, None] == slot_index[None, :]).astype(jnp.bfloat16),
        returned.reshape(slots, columns),
        preferred_element_type=jnp.float32,
    ).astype(jnp.bfloat16)
    return (new_embedding, new_state, next_rows)


def solution(mesh):
    in_specs = (
        P(("dp", "rows"), None),
        P(("dp", "rows")),
        P(("dp", "rows"), None),
        P(("dp", "rows"), None),
        P(("dp", "rows")),
        P(("dp", "rows"), None),
        P(("dp", "rows")),
    )
    out_specs = (P(("dp", "rows"), None), P(("dp", "rows")), P(("dp", "rows"), None))
    return jax.shard_map(
        on_device, mesh=mesh, in_specs=in_specs, out_specs=out_specs, check_vma=False
    )
```

```python
import jax
import jax.numpy as jnp
from jax import lax
from jax.experimental import pallas as pl
from jax.experimental.pallas import tpu as pltpu
from jax.sharding import PartitionSpec as P

BANKS = 4
LANES = 128
BASE = 256


def positions_of(owner_ids, next_ids, devices):
    lookups = owner_ids.shape[0]
    names = jnp.arange(devices, dtype=jnp.int32)[None, :]
    one_hot = jnp.concatenate(
        [owner_ids[:, None] == names, next_ids[:, None] == names], axis=1
    ).astype(jnp.bfloat16)
    index = jnp.arange(lookups, dtype=jnp.int32)
    earlier = (index[:, None] > index[None, :]).astype(jnp.bfloat16)
    ahead = jnp.dot(earlier, one_hot, preferred_element_type=jnp.float32)
    hits = ahead * one_hot.astype(jnp.float32)
    slots = jnp.sum(hits[:, :devices], axis=1), jnp.sum(hits[:, devices:], axis=1)
    return tuple(part.astype(jnp.int32) for part in slots)


def slot_table(owner_ids, slot_ids, offsets, devices, capacity):
    names = jnp.arange(devices, dtype=jnp.int32)[None, :]
    one_hot = (owner_ids[:, None] == names).astype(jnp.bfloat16)
    in_slot = slot_ids[:, None] == jnp.arange(capacity, dtype=jnp.int32)[None, :]
    high = (offsets // BASE).astype(jnp.float32)[:, None]
    low = (offsets % BASE).astype(jnp.float32)[:, None]
    columns = jnp.concatenate(
        [jnp.where(in_slot, high, 0.0), jnp.where(in_slot, low, 0.0), jnp.where(in_slot, 1.0, 0.0)],
        axis=1,
    ).astype(jnp.bfloat16)
    table = lax.dot_general(
        one_hot, columns, (((0,), (0,)), ((), ())), preferred_element_type=jnp.float32
    )
    return jnp.split(table, 3, axis=1)


def update_kernel(
    rows_hbm, wanted_hbm, incoming_ref, embedding_ref, state_ref,
    new_embedding_ref, new_state_ref, fetched_ref,
    *scratch,
):
    banks = scratch[:BANKS]
    table, picked, rows_ref, wanted_ref, in_sem, rows_sem, wanted_sem, out_sems = scratch[BANKS:]
    owned = table.shape[0]
    slots = picked.shape[0]
    blocks = incoming_ref.shape[0]
    capacity = slots // blocks
    chunks = out_sems.shape[0]
    chunk = owned // chunks

    rows_load = pltpu.make_async_copy(rows_hbm, rows_ref, rows_sem)
    rows_load.start()
    wanted_load = pltpu.make_async_copy(wanted_hbm, wanted_ref, wanted_sem)
    wanted_load.start()
    load = pltpu.make_async_copy(embedding_ref, table, in_sem)
    load.start()

    zero_rows = 128

    @pl.loop(0, owned // zero_rows)
    def _(step):
        for bank in banks:
            bank[pl.ds(pl.multiple_of(step * zero_rows, zero_rows), zero_rows), :] = jnp.zeros(
                (zero_rows, LANES), jnp.float32
            )

    group = 32 if capacity % 32 == 0 else 8
    per_block = capacity // group
    rows_load.wait()

    @pl.loop(0, blocks * per_block)
    def _(step):
        start = pl.multiple_of(step * group, group)
        within = pl.multiple_of(lax.rem(step, per_block) * group, group)
        block = incoming_ref[lax.div(step, per_block), pl.ds(within, group), :].astype(jnp.float32)
        for first in range(0, group, BANKS):
            where = [rows_ref[start + first + k] for k in range(BANKS)]
            sums = [
                banks[k][pl.ds(where[k], 1), :] + block[first + k : first + k + 1, :]
                for k in range(BANKS)
            ]
            for k in range(BANKS):
                banks[k][pl.ds(where[k], 1), :] = sums[k]

    load.wait()
    for piece in range(chunks):

        @pl.loop(0, chunk // LANES, unroll=2)
        def _(step):
            tile = piece * (chunk // LANES) + step
            span = pl.ds(pl.multiple_of(tile * LANES, LANES), LANES)
            grad_sum = banks[0][span, :]
            for bank in banks[1:]:
                grad_sum = grad_sum + bank[span, :]
            mean = jnp.sum(grad_sum * grad_sum, axis=1, keepdims=True) * (1.0 / LANES)
            old = jnp.broadcast_to(state_ref[pl.ds(tile, 1), :], (LANES, LANES)).T
            state = old + mean
            new_state_ref[pl.ds(tile, 1), :] = state.T[0:1, :]
            table[span, :] = table[span, :] - 0.5 * grad_sum * lax.rsqrt(state)

        span = pl.ds(piece * chunk, chunk)
        pltpu.make_async_copy(
            table.at[span, :], new_embedding_ref.at[span, :], out_sems.at[piece]
        ).start()

    wanted_load.wait()

    @pl.loop(0, slots // group)
    def _(step):
        start = pl.multiple_of(step * group, group)
        for k in range(group):
            picked[pl.ds(start + k, 1), :] = table[pl.ds(wanted_ref[start + k], 1), :]

    @pl.loop(0, slots // LANES)
    def _(step):
        span = pl.ds(pl.multiple_of(step * LANES, LANES), LANES)
        fetched_ref[span, :] = picked[span, :].astype(jnp.bfloat16)

    for piece in range(chunks):
        span = pl.ds(piece * chunk, chunk)
        pltpu.make_async_copy(
            table.at[span, :], new_embedding_ref.at[span, :], out_sems.at[piece]
        ).wait()


def update(rows, wanted, incoming, embedding, state):
    owned, columns = embedding.shape
    slots = rows.shape[0]
    chunks = 8
    vmem = pl.BlockSpec(memory_space=pltpu.VMEM)
    hbm = pl.BlockSpec(memory_space=pltpu.HBM)
    new_embedding, new_state, fetched = pl.pallas_call(
        update_kernel,
        name="update",
        out_shape=(
            jax.ShapeDtypeStruct((owned, columns), jnp.float32),
            jax.ShapeDtypeStruct((owned // LANES, LANES), jnp.float32),
            jax.ShapeDtypeStruct((slots, columns), jnp.bfloat16),
        ),
        in_specs=[hbm, hbm, vmem, hbm, vmem],
        out_specs=(hbm, vmem, vmem),
        scratch_shapes=[pltpu.VMEM((owned + 8, columns), jnp.float32)] * BANKS
        + [
            pltpu.VMEM((owned, columns), jnp.float32),
            pltpu.VMEM((slots, columns), jnp.float32),
            pltpu.SMEM((slots,), jnp.int32),
            pltpu.SMEM((slots,), jnp.int32),
            pltpu.SemaphoreType.DMA,
            pltpu.SemaphoreType.DMA,
            pltpu.SemaphoreType.DMA,
            pltpu.SemaphoreType.DMA((chunks,)),
        ],
        compiler_params=pltpu.CompilerParams(vmem_limit_bytes=50 * 1024 * 1024),
    )(rows, wanted, incoming, embedding, state.reshape(owned // LANES, LANES))
    return new_embedding, new_state.reshape(owned), fetched


def on_device(owners, offsets, gradients, embedding, adagrad_state, next_owners, next_offsets):
    axes = ("dp", "rows")
    devices = lax.axis_size(axes)
    lookups, columns = gradients.shape
    owned_rows = embedding.shape[0]
    capacity = max(2, 4 * lookups // devices)
    slots = devices * capacity
    owner_ids, next_ids = owners[:, 0], next_owners[:, 0]
    slot_ids, next_slots = positions_of(owner_ids, next_ids, devices)
    places = owner_ids * capacity + slot_ids
    next_places = next_ids * capacity + next_slots
    high, low, used = slot_table(owner_ids, slot_ids, offsets, devices, capacity)
    next_high, next_low, _ = slot_table(next_ids, next_slots, next_offsets, devices, capacity)
    high = jnp.where(used > 0, high, owned_rows // BASE)
    ids = jnp.concatenate([high, low, next_high, next_low], axis=1).astype(jnp.bfloat16)
    id_rows = 8 * -(-4 * capacity // (8 * columns))
    ids = jnp.pad(ids, ((0, 0), (0, id_rows * columns - 4 * capacity)))
    slot_index = jnp.arange(slots, dtype=jnp.int32)
    outgoing = jnp.dot(
        (slot_index[:, None] == places[None, :]).astype(jnp.bfloat16),
        gradients,
        preferred_element_type=jnp.float32,
    ).astype(jnp.bfloat16)
    outgoing = jnp.concatenate(
        [outgoing.reshape(devices, capacity, columns), ids.reshape(devices, id_rows, columns)], axis=1
    )
    incoming = lax.all_to_all(outgoing, axes, split_axis=0, concat_axis=0, tiled=True)
    ids = incoming[:, capacity:].reshape(devices, id_rows * columns)[:, : 4 * capacity]
    ids = ids.astype(jnp.int32).reshape(devices, 4, capacity)
    rows = (ids[:, 0] * BASE + ids[:, 1]).reshape(-1)
    wanted = (ids[:, 2] * BASE + ids[:, 3]).reshape(-1)
    new_embedding, new_state, fetched = update(rows, wanted, incoming, embedding, adagrad_state)
    returned = lax.all_to_all(
        fetched.reshape(devices, capacity, columns), axes, split_axis=0, concat_axis=0, tiled=True
    )
    next_rows = jnp.dot(
        (next_places[:, None] == slot_index[None, :]).astype(jnp.bfloat16),
        returned.reshape(slots, columns),
        preferred_element_type=jnp.float32,
    ).astype(jnp.bfloat16)
    return (new_embedding, new_state, next_rows)


def solution(mesh):
    in_specs = (
        P(("dp", "rows"), None),
        P(("dp", "rows")),
        P(("dp", "rows"), None),
        P(("dp", "rows"), None),
        P(("dp", "rows")),
        P(("dp", "rows"), None),
        P(("dp", "rows")),
    )
    out_specs = (P(("dp", "rows"), None), P(("dp", "rows")), P(("dp", "rows"), None))
    return jax.shard_map(
        on_device, mesh=mesh, in_specs=in_specs, out_specs=out_specs, check_vma=False
    )
```

```python
import jax
import jax.numpy as jnp
from jax import lax
from jax.experimental import pallas as pl
from jax.experimental.pallas import tpu as pltpu
from jax.sharding import PartitionSpec as P

BANKS = 4
LANES = 128
BASE = 256


def positions_of(owner_ids, next_ids, devices):
    lookups = owner_ids.shape[0]
    names = jnp.arange(devices, dtype=jnp.int32)[None, :]
    one_hot = jnp.concatenate(
        [owner_ids[:, None] == names, next_ids[:, None] == names], axis=1
    ).astype(jnp.bfloat16)
    index = jnp.arange(lookups, dtype=jnp.int32)
    earlier = (index[:, None] > index[None, :]).astype(jnp.bfloat16)
    ahead = jnp.dot(earlier, one_hot, preferred_element_type=jnp.float32)
    hits = ahead * one_hot.astype(jnp.float32)
    slots = jnp.sum(hits[:, :devices], axis=1), jnp.sum(hits[:, devices:], axis=1)
    return tuple(part.astype(jnp.int32) for part in slots)


def slot_table(owner_ids, slot_ids, offsets, devices, capacity):
    names = jnp.arange(devices, dtype=jnp.int32)[None, :]
    one_hot = (owner_ids[:, None] == names).astype(jnp.bfloat16)
    in_slot = slot_ids[:, None] == jnp.arange(capacity, dtype=jnp.int32)[None, :]
    high = (offsets // BASE).astype(jnp.float32)[:, None]
    low = (offsets % BASE).astype(jnp.float32)[:, None]
    columns = jnp.concatenate(
        [jnp.where(in_slot, high, 0.0), jnp.where(in_slot, low, 0.0), jnp.where(in_slot, 1.0, 0.0)],
        axis=1,
    ).astype(jnp.bfloat16)
    table = lax.dot_general(
        one_hot, columns, (((0,), (0,)), ((), ())), preferred_element_type=jnp.float32
    )
    return jnp.split(table, 3, axis=1)


def update_kernel(
    rows_hbm, wanted_hbm, incoming_ref, embedding_ref, state_ref,
    new_embedding_ref, new_state_ref, fetched_ref,
    *scratch,
):
    banks = scratch[:BANKS]
    table, picked, rows_ref, wanted_ref, in_sem, rows_sem, wanted_sem, out_sems = scratch[BANKS:]
    owned = table.shape[0]
    slots = picked.shape[0]
    blocks = incoming_ref.shape[0]
    capacity = slots // blocks
    chunks = out_sems.shape[0]
    chunk = owned // chunks

    rows_load = pltpu.make_async_copy(rows_hbm, rows_ref, rows_sem)
    rows_load.start()
    wanted_load = pltpu.make_async_copy(wanted_hbm, wanted_ref, wanted_sem)
    wanted_load.start()
    load = pltpu.make_async_copy(embedding_ref, table, in_sem)
    load.start()

    zero_rows = 128

    @pl.loop(0, owned // zero_rows)
    def _(step):
        for bank in banks:
            bank[pl.ds(pl.multiple_of(step * zero_rows, zero_rows), zero_rows), :] = jnp.zeros(
                (zero_rows, LANES), jnp.float32
            )

    group = next(size for size in (64, 32, 8) if capacity % size == 0)
    per_block = capacity // group
    rows_load.wait()

    @pl.loop(0, blocks * per_block)
    def _(step):
        start = pl.multiple_of(step * group, group)
        within = pl.multiple_of(lax.rem(step, per_block) * group, group)
        block = incoming_ref[lax.div(step, per_block), pl.ds(within, group), :].astype(jnp.float32)
        for first in range(0, group, BANKS):
            where = [rows_ref[start + first + k] for k in range(BANKS)]
            sums = [
                banks[k][pl.ds(where[k], 1), :] + block[first + k : first + k + 1, :]
                for k in range(BANKS)
            ]
            for k in range(BANKS):
                banks[k][pl.ds(where[k], 1), :] = sums[k]

    load.wait()
    for piece in range(chunks):

        @pl.loop(0, chunk // LANES, unroll=4)
        def _(step):
            tile = piece * (chunk // LANES) + step
            span = pl.ds(pl.multiple_of(tile * LANES, LANES), LANES)
            grad_sum = banks[0][span, :]
            for bank in banks[1:]:
                grad_sum = grad_sum + bank[span, :]
            mean = jnp.sum(grad_sum * grad_sum, axis=1, keepdims=True) * (1.0 / LANES)
            old = jnp.broadcast_to(state_ref[pl.ds(tile, 1), :], (LANES, LANES)).T
            state = old + mean
            new_state_ref[pl.ds(tile, 1), :] = state.T[0:1, :]
            table[span, :] = table[span, :] - 0.5 * grad_sum * lax.rsqrt(state)

        span = pl.ds(piece * chunk, chunk)
        pltpu.make_async_copy(
            table.at[span, :], new_embedding_ref.at[span, :], out_sems.at[piece]
        ).start()

    wanted_load.wait()

    @pl.loop(0, slots // group)
    def _(step):
        start = pl.multiple_of(step * group, group)
        for k in range(group):
            picked[pl.ds(start + k, 1), :] = table[pl.ds(wanted_ref[start + k], 1), :]

    @pl.loop(0, slots // LANES)
    def _(step):
        span = pl.ds(pl.multiple_of(step * LANES, LANES), LANES)
        fetched_ref[span, :] = picked[span, :].astype(jnp.bfloat16)

    for piece in range(chunks):
        span = pl.ds(piece * chunk, chunk)
        pltpu.make_async_copy(
            table.at[span, :], new_embedding_ref.at[span, :], out_sems.at[piece]
        ).wait()


def update(rows, wanted, incoming, embedding, state):
    owned, columns = embedding.shape
    slots = rows.shape[0]
    chunks = 8
    vmem = pl.BlockSpec(memory_space=pltpu.VMEM)
    hbm = pl.BlockSpec(memory_space=pltpu.HBM)
    new_embedding, new_state, fetched = pl.pallas_call(
        update_kernel,
        name="update",
        out_shape=(
            jax.ShapeDtypeStruct((owned, columns), jnp.float32),
            jax.ShapeDtypeStruct((owned // LANES, LANES), jnp.float32),
            jax.ShapeDtypeStruct((slots, columns), jnp.bfloat16),
        ),
        in_specs=[hbm, hbm, vmem, hbm, vmem],
        out_specs=(hbm, vmem, vmem),
        scratch_shapes=[pltpu.VMEM((owned + 8, columns), jnp.float32)] * BANKS
        + [
            pltpu.VMEM((owned, columns), jnp.float32),
            pltpu.VMEM((slots, columns), jnp.float32),
            pltpu.SMEM((slots,), jnp.int32),
            pltpu.SMEM((slots,), jnp.int32),
            pltpu.SemaphoreType.DMA,
            pltpu.SemaphoreType.DMA,
            pltpu.SemaphoreType.DMA,
            pltpu.SemaphoreType.DMA((chunks,)),
        ],
        compiler_params=pltpu.CompilerParams(vmem_limit_bytes=50 * 1024 * 1024),
    )(rows, wanted, incoming, embedding, state.reshape(owned // LANES, LANES))
    return new_embedding, new_state.reshape(owned), fetched


def on_device(owners, offsets, gradients, embedding, adagrad_state, next_owners, next_offsets):
    axes = ("dp", "rows")
    devices = lax.axis_size(axes)
    lookups, columns = gradients.shape
    owned_rows = embedding.shape[0]
    capacity = max(2, 4 * lookups // devices)
    slots = devices * capacity
    owner_ids, next_ids = owners[:, 0], next_owners[:, 0]
    slot_ids, next_slots = positions_of(owner_ids, next_ids, devices)
    places = owner_ids * capacity + slot_ids
    next_places = next_ids * capacity + next_slots
    high, low, used = slot_table(owner_ids, slot_ids, offsets, devices, capacity)
    next_high, next_low, _ = slot_table(next_ids, next_slots, next_offsets, devices, capacity)
    high = jnp.where(used > 0, high, owned_rows // BASE)
    ids = jnp.concatenate([high, low, next_high, next_low], axis=1).astype(jnp.bfloat16)
    id_rows = 8 * -(-4 * capacity // (8 * columns))
    ids = jnp.pad(ids, ((0, 0), (0, id_rows * columns - 4 * capacity)))
    slot_index = jnp.arange(slots, dtype=jnp.int32)
    outgoing = jnp.dot(
        (slot_index[:, None] == places[None, :]).astype(jnp.bfloat16),
        gradients,
        preferred_element_type=jnp.float32,
    ).astype(jnp.bfloat16)
    outgoing = jnp.concatenate(
        [outgoing.reshape(devices, capacity, columns), ids.reshape(devices, id_rows, columns)], axis=1
    )
    incoming = lax.all_to_all(outgoing, axes, split_axis=0, concat_axis=0, tiled=True)
    ids = incoming[:, capacity:].reshape(devices, id_rows * columns)[:, : 4 * capacity]
    ids = ids.astype(jnp.int32).reshape(devices, 4, capacity)
    rows = (ids[:, 0] * BASE + ids[:, 1]).reshape(-1)
    wanted = (ids[:, 2] * BASE + ids[:, 3]).reshape(-1)
    new_embedding, new_state, fetched = update(rows, wanted, incoming, embedding, adagrad_state)
    returned = lax.all_to_all(
        fetched.reshape(devices, capacity, columns), axes, split_axis=0, concat_axis=0, tiled=True
    )
    next_rows = jnp.dot(
        (next_places[:, None] == slot_index[None, :]).astype(jnp.bfloat16),
        returned.reshape(slots, columns),
        preferred_element_type=jnp.float32,
    ).astype(jnp.bfloat16)
    return (new_embedding, new_state, next_rows)


def solution(mesh):
    in_specs = (
        P(("dp", "rows"), None),
        P(("dp", "rows")),
        P(("dp", "rows"), None),
        P(("dp", "rows"), None),
        P(("dp", "rows")),
        P(("dp", "rows"), None),
        P(("dp", "rows")),
    )
    out_specs = (P(("dp", "rows"), None), P(("dp", "rows")), P(("dp", "rows"), None))
    return jax.shard_map(
        on_device, mesh=mesh, in_specs=in_specs, out_specs=out_specs, check_vma=False
    )
```
